256 devices in a mesh: grp: 16 (over x, y), dev: 16 (over z, core).
Axes of the slice: x: 4, y: 4, z: 8, core: 2. Of those that a mesh axis runs over, the one named last changes fastest.
Arguments:
- acts: bfloat16 [65536, 12288], P(('grp', 'dev')), may hold values from -6 to 6
- grads_out: bfloat16 [65536, 64], P(('grp', 'dev')), may hold values from -0.375 to 0.375
- residual_in: float32 [256, 64, 12288], P(('grp', 'dev')), may hold values from -6 to 6
- sel_index: int32 [256, 64], P(('grp', 'dev')), may hold values from 0 to 6143, as said below
- sel_count: int32 [256], P(('grp', 'dev')), may hold values from 16 to 64, as said below
- momentum_in: float32 [64, 12288], P(None, 'dev'), may hold values from -6 to 6
Outputs:
- residual_out: float32 [256, 64, 12288], P(('grp', 'dev'))
- momentum_out: float32 [64, 12288], P(None, 'dev')
The draws below stay inside these ranges and needn't reach their ends.
Inputs may be any that keep to these rules, and one draw needn't show every extreme that they name: `sel_index`: the 64 numbers of a row are distinct. `sel_count`: equal to 64 on some device in every draw.
All inputs are finite; a program needn't handle non-finite values.
Results may differ from the reference program's by a relative error of at most 0.0003.
Values sent between devices are 32-bit elements; how exact they have to be, the bound alone decides.
No kernel may reach another device: no remote copies, remote signals or barrier semaphores. Data moves between devices by JAX's collectives and lax.ppermute only.
A program may use at most 64 MiB of HBM per device.

```python
import jax
import jax.numpy as jnp
from jax import lax

D = 12288
COLS = 64
TOK_DEV = 256
KSEL = 64
NBLK = 6144
TOKENS = 65536
DEVICES = 256


def draw_sel_index(key, part):
    keys = jax.random.split(jax.random.fold_in(key, 11), DEVICES)

    def one_row(row_key):
        return jax.random.permutation(row_key, NBLK)[:KSEL]
    return jax.vmap(one_row)(keys).astype(jnp.int32)


def draw_sel_count(key, part):
    counts = jax.random.randint(jax.random.fold_in(key, 23), (DEVICES,), KSEL // 4, KSEL + 1)
    fullest = jax.random.randint(jax.random.fold_in(key, 29), (), 0, DEVICES)
    return counts.at[fullest].set(KSEL).astype(jnp.int32)


def shard_levels(key, dims, pieces, least, largest):
    def one(axis_at, shards_of):
        steps = jax.random.uniform(jax.random.fold_in(jax.random.fold_in(key, 6), axis_at), (shards_of,), jnp.float32, least / len(pieces), largest / len(pieces))
        return jnp.repeat(jnp.exp(steps), dims[axis_at] // shards_of).reshape((-1,) + (1,) * (len(dims) - axis_at - 1))

    gain = one(*pieces[0])
    for cut in pieces[1:]:
        gain = gain * one(*cut)
    return gain


def centred(stream_key, dims, scale, limit, cuts=(), held_as=jnp.bfloat16):
    result = scale * jax.random.normal(stream_key, dims, jnp.float32)
    if cuts:
        result = result * shard_levels(stream_key, dims, cuts, -0.22, 0.18)
    return jnp.clip(result, -limit, limit).astype(held_as)


def setup_inputs(seed: int = 0) -> dict:
    splits = jax.random.split(jax.random.key(seed), 7)
    acts = centred(splits[0], (TOKENS, D), 1.0, 6.0, ((0, 256),))
    grads_out = centred(splits[1], (TOKENS, COLS), TOK_DEV ** -0.5, 0.375, ((0, 256),))
    residual_in = centred(splits[2], (DEVICES, COLS, D), 1.0, 6.0, ((0, 256),), jnp.float32)
    sel_index = draw_sel_index(jax.random.fold_in(splits[6], 71), 0)
    sel_count = draw_sel_count(jax.random.fold_in(splits[6], 71), 0)
    momentum_in = centred(splits[5], (COLS, D), 1.0, 6.0, ((1, 16),), jnp.float32)
    return {"acts": acts, "grads_out": grads_out, "residual_in": residual_in, "sel_index": sel_index, "sel_count": sel_count, "momentum_in": momentum_in}


def one_device(operands):
    inputs, out_grads, residual, chosen, how_many = operands
    local_grad = lax.dot_general(out_grads, inputs, (((0,), (0,)), ((), ())), preferred_element_type=jnp.float32)
    summed = residual + local_grad
    blocks = summed.reshape(NBLK, 128)
    valid_rows = (jnp.arange(KSEL, dtype=jnp.int32) < how_many).astype(jnp.float32)
    picked = blocks[chosen] * valid_rows[:, None]
    marked = jnp.zeros((NBLK,), jnp.float32).at[chosen].max(valid_rows)
    kept = blocks * (1.0 - marked)[:, None]
    return kept.reshape(COLS, D), picked


def reference(acts, grads_out, residual_in, sel_index, sel_count, momentum_in):
    inputs = acts.reshape(DEVICES, TOK_DEV, D)
    out_grads = grads_out.reshape(DEVICES, TOK_DEV, COLS)
    residual_out, picked = lax.map(one_device, (inputs, out_grads, residual_in, sel_index, sel_count))
    spread = jnp.zeros((NBLK, 128), jnp.float32).at[sel_index.reshape(-1)].add(picked.reshape(-1, 128))
    momentum_out = 0.9 * momentum_in + spread.reshape(COLS, D)
    return residual_out, momentum_out
```

```python
import jax
import jax.numpy as jnp
from jax import lax
from jax.experimental import pallas as pl
from jax.experimental.pallas import tpu as pltpu
from jax.sharding import PartitionSpec as P

momentum_decay = 0.9
lanes = 128
sublanes = 8
chunk_count = 8


def pick_kernel(index_s, count_s, index_v, grads_t, acts, residual, grad_ref, out_ref,
                acts_v, tiles, codes_v, acts_sems, tile_sem, *, row_blocks, own_blocks):
    row_tiles = grad_ref.shape[0]
    slots = index_s.shape[1]
    chunk = row_blocks * lanes // chunk_count
    chunk_blocks = row_blocks // chunk_count
    members = out_ref.shape[0]
    half = own_blocks // 2
    part = half * sublanes

    def acts_copy(i):
        at = pl.ds(pl.multiple_of(i * chunk, lanes), chunk)
        return pltpu.make_async_copy(acts.at[:, at], acts_v.at[i], acts_sems.at[i])

    for i in range(chunk_count):
        acts_copy(i).start()

    def fetch(s, carry):
        block = index_s[0, s]
        row = block // row_blocks
        col = block - row * row_blocks
        pltpu.make_async_copy(residual.at[row // sublanes, col], tiles.at[s], tile_sem).start()
        return carry

    lax.fori_loop(0, slots, fetch, 0, unroll=8)

    count = count_s[0]
    block = index_v[...]
    row = (block * 43691) >> 22
    col = block - row * row_blocks
    owner = (col * 10923) >> 16
    inner = col - owner * own_blocks
    side = jnp.where(inner >= half, 1, 0)
    share = (row >> 3) * 2 + side
    target = owner * part + (inner - side * half) * sublanes + (row & 7)
    code = share * (part * row_blocks // own_blocks) + target
    slot = lax.broadcasted_iota(jnp.int32, code.shape, 1)
    code = jnp.where(slot < count, code, -1).astype(jnp.float32)
    codes_v[...] = jnp.zeros_like(codes_v)
    codes_v[0:1, 0:slots] = code
    both = codes_v[...]
    both = both + pltpu.roll(both, slots, 1)
    out_ref[0, slots:slots + sublanes, :] = both

    def multiply(i, carry):
        acts_copy(i).wait()
        grad = jnp.dot(grads_t[...], acts_v[i], preferred_element_type=jnp.float32)
        for r in range(row_tiles):
            for c in range(chunk_blocks):
                grad_ref[r, i * chunk_blocks + c] = grad[
                    r * sublanes:(r + 1) * sublanes, c * lanes:(c + 1) * lanes
                ]
        return carry

    lax.fori_loop(0, chunk_count, multiply, 0)
    pltpu.make_async_copy(tiles, tiles, tile_sem).wait()

    def pick(s, carry):
        block = index_s[0, s]
        row = block // row_blocks
        col = block - row * row_blocks
        mine = jnp.logical_and(sub == row % sublanes, s < count)
        held = tiles[s]
        grad = grad_ref[row // sublanes, col]
        grad_ref[row // sublanes, col] = jnp.where(mine, -held, grad)
        tiles[s] = jnp.where(mine, held + grad, 0.0)
        out_ref[0, pl.ds(s, 1), :] = tiles[s, pl.ds(row % sublanes, 1), :]
        return carry

    sub = lax.broadcasted_iota(jnp.int32, (sublanes, lanes), 0)

    lax.fori_loop(0, slots, pick, 0, unroll=8)
    message = out_ref[0]
    for j in range(1, members):
        out_ref[j] = message


def add_kernel(held, out_ref, *, slots):
    sources = held.shape[0]
    rows = out_ref.shape[0]
    base = lax.axis_index("grp") * rows
    target = (lax.broadcasted_iota(jnp.int32, (rows, lanes), 0) + base).astype(jnp.float32)
    low = lax.broadcasted_iota(jnp.int32, (1, lanes), 1) < slots
    total = jnp.zeros((rows, 2 * lanes), jnp.float32)
    for q in range(0, sources, 4):
        hits = []
        for p in (q, q + 2):
            code = jnp.where(low, held[p, slots:slots + 1, :], held[p + 1, slots:slots + 1, :])
            hits.append(jnp.where(target == code, 1.0, 0.0).astype(jnp.bfloat16))
        values = jnp.concatenate([held[p, 0:slots, :] for p in range(q, q + 4)], axis=0)
        high = values.astype(jnp.bfloat16)
        rest = (values - high.astype(jnp.float32)).astype(jnp.bfloat16)
        total = total + jnp.dot(
            jnp.concatenate(hits, axis=1),
            jnp.concatenate([high, rest], axis=1),
            preferred_element_type=jnp.float32,
        )
    out_ref[...] = total[:, :lanes] + total[:, lanes:]


def final_kernel(parts, momentum, out_ref):
    members, part, _ = out_ref.shape
    wide = part // sublanes * lanes
    me = lax.axis_index("grp")
    total = parts[0]
    for j in range(1, members):
        total = total + parts[j]
    rows = pl.ds(pl.multiple_of((me // 2) * sublanes, sublanes), sublanes)
    old = momentum[rows, pl.ds(pl.multiple_of((me % 2) * wide, lanes), wide)]
    for c in range(part // sublanes):
        at = slice(c * sublanes, (c + 1) * sublanes)
        new = momentum_decay * old[:, c * lanes:(c + 1) * lanes] + total[at]
        for j in range(members):
            out_ref[j, at, :] = new


def keep_kernel(grad, residual, out_ref):
    i = pl.program_id(0)
    for c in range(grad.shape[1]):
        at = slice(c * lanes, (c + 1) * lanes)
        out_ref[0, :, at] = residual[0, :, at] + grad[i, c]


def local(acts, grads_out, residual_in, sel_index, sel_count, momentum_in):
    tokens, width = acts.shape
    columns = grads_out.shape[1]
    slots = sel_index.shape[1]
    row_blocks = width // lanes
    own_blocks = momentum_in.shape[1] // lanes
    members = lax.axis_size("grp")
    owners = lax.axis_size("dev")
    part = own_blocks // 2 * sublanes
    smem = pl.BlockSpec(memory_space=pltpu.SMEM)
    vmem = pl.BlockSpec(memory_space=pltpu.VMEM)
    hbm = pl.BlockSpec(memory_space=pl.ANY)
    tiled = residual_in.reshape(columns // sublanes, sublanes, row_blocks, lanes)
    tiled = tiled.transpose(0, 2, 1, 3)

    def pick(*refs):
        pick_kernel(*refs, row_blocks=row_blocks, own_blocks=own_blocks)

    grad, message = pl.pallas_call(
        pick,
        in_specs=[smem, smem, vmem, vmem, hbm, hbm],
        out_specs=[vmem, vmem],
        out_shape=[
            pltpu.VMEM(tiled.shape, jnp.float32),
            pltpu.VMEM((members, slots + sublanes, lanes), jnp.float32),
        ],
        scratch_shapes=[
            pltpu.VMEM((chunk_count, tokens, width // chunk_count), jnp.bfloat16),
            pltpu.VMEM((slots, sublanes, lanes), jnp.float32),
            pltpu.VMEM((sublanes, lanes), jnp.float32),
            pltpu.SemaphoreType.DMA((chunk_count,)),
            pltpu.SemaphoreType.DMA,
        ],
        compiler_params=pltpu.CompilerParams(vmem_limit_bytes=16 << 20),
        name="pick",
    )(
        sel_index, sel_count, sel_index, grads_out.T,
        pltpu.with_memory_space_constraint(acts, pltpu.HBM),
        pltpu.with_memory_space_constraint(tiled, pltpu.HBM),
    )

    held = lax.all_to_all(message, "grp", 0, 0, tiled=True)

    sums = pl.pallas_call(
        lambda *refs: add_kernel(*refs, slots=slots),
        in_specs=[vmem],
        out_specs=vmem,
        out_shape=pltpu.VMEM((owners * part, lanes), jnp.float32),
        compiler_params=pltpu.CompilerParams(vmem_limit_bytes=8 << 20),
        name="add",
    )(held)
    parts = lax.all_to_all(sums.reshape(owners, part, lanes), "dev", 0, 0, tiled=True)

    new = pl.pallas_call(
        final_kernel,
        in_specs=[vmem, vmem],
        out_specs=vmem,
        out_shape=pltpu.VMEM((members, part, lanes), jnp.float32),
        compiler_params=pltpu.CompilerParams(vmem_limit_bytes=8 << 20),
        name="final",
    )(parts, momentum_in)
    whole = lax.all_to_all(new, "grp", 0, 0, tiled=True)
    whole = whole.reshape(columns // sublanes, 2, own_blocks // 2, sublanes, lanes)
    whole = whole.transpose(0, 3, 1, 2, 4).reshape(columns, own_blocks * lanes)
    block = pl.BlockSpec((1, sublanes, width), lambda i: (0, i, 0))
    kept = pl.pallas_call(
        keep_kernel,
        grid=(columns // sublanes,),
        in_specs=[vmem, block],
        out_specs=block,
        out_shape=jax.ShapeDtypeStruct(residual_in.shape, jnp.float32),
        compiler_params=pltpu.CompilerParams(vmem_limit_bytes=8 << 20),
        name="keep",
    )(
        pltpu.with_memory_space_constraint(grad, pltpu.VMEM),
        pltpu.with_memory_space_constraint(residual_in, pltpu.HBM),
    )
    return (kept, whole)


def solution(mesh):
    placed = (
        P(("grp", "dev"), None),
        P(("grp", "dev"), None),
        P(("grp", "dev"), None, None),
        P(("grp", "dev"), None),
        P(("grp", "dev")),
        P(None, "dev"),
    )
    return jax.shard_map(
        local,
        mesh=mesh,
        in_specs=placed,
        out_specs=(P(("grp", "dev"), None, None), P(None, "dev")),
        check_vma=False,
    )
```

```python
import jax
import jax.numpy as jnp
from jax import lax
from jax.experimental import pallas as pl
from jax.experimental.pallas import tpu as pltpu
from jax.sharding import PartitionSpec as P

momentum_decay = 0.9
lanes = 128
sublanes = 8
chunk_count = 3


def pick_kernel(index, count_s, grads_t, acts, residual, grad_ref, out_ref,
                index_s, index_v, grads_v, acts_v, tiles, codes_v,
                small_sems, acts_sems, tile_sem, *, row_blocks, own_blocks):
    row_tiles = grad_ref.shape[0]
    slots = index.shape[1]
    members = out_ref.shape[0]
    half = own_blocks // 2
    part = half * sublanes
    chunk_blocks = row_blocks // chunk_count
    chunk = chunk_blocks * lanes

    scalars = pltpu.make_async_copy(index, index_s, small_sems.at[0])
    vector = pltpu.make_async_copy(index, index_v, small_sems.at[1])
    left = pltpu.make_async_copy(grads_t, grads_v, small_sems.at[2])
    chunks = [
        pltpu.make_async_copy(
            acts.at[:, i * chunk:(i + 1) * chunk],
            acts_v.at[:, i * chunk:(i + 1) * chunk],
            acts_sems.at[i],
        )
        for i in range(chunk_count)
    ]
    scalars.start()
    left.start()
    chunks[0].start()
    vector.start()
    for copy in chunks[1:]:
        copy.start()

    def place(s):
        block = index_s[0, s]
        row = block // row_blocks
        return row // sublanes, row % sublanes, block - row * row_blocks

    def fetch(s, carry):
        high, _, col = place(s)
        pltpu.make_async_copy(residual.at[high, col], tiles.at[s], tile_sem).start()
        return carry

    scalars.wait()
    lax.fori_loop(0, slots, fetch, 0, unroll=8)

    count = count_s[0]
    vector.wait()
    block = index_v[...]
    row = (block * 43691) >> 22
    col = block - row * row_blocks
    owner = (col * 10923) >> 16
    inner = col - owner * own_blocks
    side = jnp.where(inner >= half, 1, 0)
    share = (row >> 3) * 2 + side
    target = owner * part + (inner - side * half) * sublanes + (row & 7)
    code = share * (part * row_blocks // own_blocks) + target
    slot = lax.broadcasted_iota(jnp.int32, code.shape, 1)
    code = jnp.where(slot < count, code, -1).astype(jnp.float32)
    codes_v[...] = jnp.zeros_like(codes_v)
    codes_v[0:1, 0:slots] = code
    both = codes_v[...]
    both = both + pltpu.roll(both, slots, 1)
    out_ref[0, slots:slots + sublanes, :] = both

    left.wait()
    for i in range(chunk_count):
        chunks[i].wait()
        grad = jnp.dot(
            grads_v[...],
            acts_v[:, i * chunk:(i + 1) * chunk],
            preferred_element_type=jnp.float32,
        )
        for r in range(row_tiles):
            for c in range(chunk_blocks):
                grad_ref[r, i * chunk_blocks + c] = grad[
                    r * sublanes:(r + 1) * sublanes, c * lanes:(c + 1) * lanes
                ]
    pltpu.make_async_copy(tiles, tiles, tile_sem).wait()

    sub = lax.broadcasted_iota(jnp.int32, (sublanes, lanes), 0)

    def pick(s, carry):
        high, low, col = place(s)
        mine = jnp.logical_and(sub == low, s < count)
        held = tiles[s]
        grad = grad_ref[high, col]
        grad_ref[high, col] = jnp.where(mine, -held, grad)
        tiles[s] = jnp.where(mine, held + grad, 0.0)
        out_ref[0, pl.ds(s, 1), :] = tiles[s, pl.ds(low, 1), :]
        return carry

    lax.fori_loop(0, slots, pick, 0, unroll=8)
    message = out_ref[0]
    for j in range(1, members):
        out_ref[j] = message


def add_kernel(held, out_ref, *, slots):
    sources = held.shape[0]
    rows = out_ref.shape[0]
    base = lax.axis_index("grp") * rows
    target = (lax.broadcasted_iota(jnp.int32, (rows, lanes), 0) + base).astype(jnp.float32)
    low = lax.broadcasted_iota(jnp.int32, (1, lanes), 1) < slots
    total = jnp.zeros((rows, 2 * lanes), jnp.float32)
    for q in range(0, sources, 4):
        hits = []
        for p in (q, q + 2):
            code = jnp.where(low, held[p, slots:slots + 1, :], held[p + 1, slots:slots + 1, :])
            hits.append(jnp.where(target == code, 1.0, 0.0).astype(jnp.bfloat16))
        values = jnp.concatenate([held[p, 0:slots, :] for p in range(q, q + 4)], axis=0)
        high = values.astype(jnp.bfloat16)
        rest = (values - high.astype(jnp.float32)).astype(jnp.bfloat16)
        total = total + jnp.dot(
            jnp.concatenate(hits, axis=1),
            jnp.concatenate([high, rest], axis=1),
            preferred_element_type=jnp.float32,
        )
    out_ref[...] = total[:, :lanes] + total[:, lanes:]


def final_kernel(parts, momentum, out_ref):
    members, part, _ = out_ref.shape
    wide = part // sublanes * lanes
    me = lax.axis_index("grp")
    total = parts[0]
    for j in range(1, members):
        total = total + parts[j]
    rows = pl.ds(pl.multiple_of((me // 2) * sublanes, sublanes), sublanes)
    old = momentum[rows, pl.ds(pl.multiple_of((me % 2) * wide, lanes), wide)]
    for c in range(part // sublanes):
        at = slice(c * sublanes, (c + 1) * sublanes)
        new = momentum_decay * old[:, c * lanes:(c + 1) * lanes] + total[at]
        for j in range(members):
            out_ref[j, at, :] = new


def keep_kernel(grad, residual, out_ref, held, in_sems, out_sems):
    row_tiles, row_blocks, _, _ = grad.shape
    reads = [
        pltpu.make_async_copy(residual.at[i], held.at[i], in_sems.at[i])
        for i in range(row_tiles)
    ]
    writes = [
        pltpu.make_async_copy(held.at[i], out_ref.at[i], out_sems.at[i])
        for i in range(row_tiles)
    ]
    for copy in reads:
        copy.start()
    for i in range(row_tiles):
        reads[i].wait()

        def add(c, carry):
            held[i, c] = held[i, c] + grad[i, c]
            return carry

        lax.fori_loop(0, row_blocks, add, 0, unroll=16)
        writes[i].start()
    for copy in writes:
        copy.wait()


def in_hbm(array):
    return pltpu.with_memory_space_constraint(array, pltpu.HBM)


def local(acts, grads_out, residual_in, sel_index, sel_count, momentum_in):
    tokens, width = acts.shape
    columns = grads_out.shape[1]
    slots = sel_index.shape[1]
    row_blocks = width // lanes
    own_blocks = momentum_in.shape[1] // lanes
    members = lax.axis_size("grp")
    owners = lax.axis_size("dev")
    part = own_blocks // 2 * sublanes
    smem = pl.BlockSpec(memory_space=pltpu.SMEM)
    vmem = pl.BlockSpec(memory_space=pltpu.VMEM)
    hbm = pl.BlockSpec(memory_space=pl.ANY)
    tiled = residual_in.reshape(columns // sublanes, sublanes, row_blocks, lanes)
    tiled = tiled.transpose(0, 2, 1, 3)

    def pick(*refs):
        pick_kernel(*refs, row_blocks=row_blocks, own_blocks=own_blocks)

    grad, message = pl.pallas_call(
        pick,
        in_specs=[hbm, smem, hbm, hbm, hbm],
        out_specs=[vmem, vmem],
        out_shape=[
            pltpu.VMEM(tiled.shape, jnp.float32),
            pltpu.VMEM((members, slots + sublanes, lanes), jnp.float32),
        ],
        scratch_shapes=[
            pltpu.SMEM((1, slots), jnp.int32),
            pltpu.VMEM((1, slots), jnp.int32),
            pltpu.VMEM((columns, tokens), jnp.bfloat16),
            pltpu.VMEM((tokens, width), jnp.bfloat16),
            pltpu.VMEM((slots, sublanes, lanes), jnp.float32),
            pltpu.VMEM((sublanes, lanes), jnp.float32),
            pltpu.SemaphoreType.DMA((3,)),
            pltpu.SemaphoreType.DMA((chunk_count,)),
            pltpu.SemaphoreType.DMA,
        ],
        compiler_params=pltpu.CompilerParams(vmem_limit_bytes=16 << 20),
        name="pick",
    )(
        in_hbm(sel_index), sel_count, in_hbm(grads_out.T), in_hbm(acts), in_hbm(tiled),
    )

    held = lax.all_to_all(message, "grp", 0, 0, tiled=True)

    sums = pl.pallas_call(
        lambda *refs: add_kernel(*refs, slots=slots),
        in_specs=[vmem],
        out_specs=vmem,
        out_shape=pltpu.VMEM((owners * part, lanes), jnp.float32),
        compiler_params=pltpu.CompilerParams(vmem_limit_bytes=8 << 20),
        name="add",
    )(held)
    parts = lax.all_to_all(sums.reshape(owners, part, lanes), "dev", 0, 0, tiled=True)

    new = pl.pallas_call(
        final_kernel,
        in_specs=[vmem, vmem],
        out_specs=vmem,
        out_shape=pltpu.VMEM((members, part, lanes), jnp.float32),
        compiler_params=pltpu.CompilerParams(vmem_limit_bytes=8 << 20),
        name="final",
    )(parts, momentum_in)
    whole = lax.all_to_all(new, "grp", 0, 0, tiled=True)
    whole = whole.reshape(columns // sublanes, 2, own_blocks // 2, sublanes, lanes)
    whole = whole.transpose(0, 3, 1, 2, 4).reshape(columns, own_blocks * lanes)
    kept = pl.pallas_call(
        keep_kernel,
        in_specs=[vmem, hbm],
        out_specs=hbm,
        out_shape=pltpu.HBM(tiled.shape, jnp.float32),
        scratch_shapes=[
            pltpu.VMEM(tiled.shape, jnp.float32),
            pltpu.SemaphoreType.DMA((tiled.shape[0],)),
            pltpu.SemaphoreType.DMA((tiled.shape[0],)),
        ],
        compiler_params=pltpu.CompilerParams(vmem_limit_bytes=8 << 20),
        name="keep",
    )(pltpu.with_memory_space_constraint(grad, pltpu.VMEM), in_hbm(tiled))
    kept = kept.transpose(0, 2, 1, 3).reshape(residual_in.shape)
    return (kept, whole)


def solution(mesh):
    placed = (
        P(("grp", "dev"), None),
        P(("grp", "dev"), None),
        P(("grp", "dev"), None, None),
        P(("grp", "dev"), None),
        P(("grp", "dev")),
        P(None, "dev"),
    )
    return jax.shard_map(
        local,
        mesh=mesh,
        in_specs=placed,
        out_specs=(P(("grp", "dev"), None, None), P(None, "dev")),
        check_vma=False,
    )
```

```python
import jax
import jax.numpy as jnp
from jax import lax
from jax.experimental import pallas as pl
from jax.experimental.pallas import tpu as pltpu
from jax.sharding import Mesh
from jax.sharding import PartitionSpec as P

momentum_decay = 0.9
lanes = 128
sublanes = 8
chunk_count = 3


def pick_kernel(index, count_s, grads_t, acts, residual, kept_ref, out_ref,
                index_s, index_v, grads_v, acts_v, residual_v, codes_v,
                small_sems, acts_sems, residual_sems, *, row_blocks, own_blocks):
    row_tiles = kept_ref.shape[0]
    slots = index.shape[1]
    rows = slots + 1
    members = out_ref.shape[0] // rows
    half = own_blocks // 2
    part = half * sublanes
    chunk_blocks = row_blocks // chunk_count
    chunk = chunk_blocks * lanes

    scalars = pltpu.make_async_copy(index, index_s, small_sems.at[0])
    vector = pltpu.make_async_copy(index, index_v, small_sems.at[1])
    left = pltpu.make_async_copy(grads_t, grads_v, small_sems.at[2])
    chunks = [
        pltpu.make_async_copy(
            acts.at[:, i * chunk:(i + 1) * chunk],
            acts_v.at[:, i * chunk:(i + 1) * chunk],
            acts_sems.at[i],
        )
        for i in range(chunk_count)
    ]
    addends = [
        pltpu.make_async_copy(
            residual.at[:, i * chunk_blocks:(i + 1) * chunk_blocks],
            residual_v.at[:, i * chunk_blocks:(i + 1) * chunk_blocks],
            residual_sems.at[i],
        )
        for i in range(chunk_count)
    ]
    left.start()
    chunks[0].start()
    vector.start()
    scalars.start()
    for i in range(chunk_count):
        if i + 1 < chunk_count:
            chunks[i + 1].start()
        addends[i].start()

    count = count_s[0]
    vector.wait()
    block = index_v[...]
    row = (block * 43691) >> 22
    col = block - row * row_blocks
    owner = (col * 10923) >> 16
    inner = col - owner * own_blocks
    side = jnp.where(inner >= half, 1, 0)
    share = (row >> 3) * 2 + side
    target = owner * part + (inner - side * half) * sublanes + (row & 7)
    code = share * (part * row_blocks // own_blocks) + target
    slot = lax.broadcasted_iota(jnp.int32, code.shape, 1)
    code = jnp.where(slot < count, code, -1).astype(jnp.float32)
    codes_v[...] = jnp.zeros_like(codes_v)
    codes_v[0:1, 0:slots] = code
    both = codes_v[...]
    both = both + pltpu.roll(both, slots, 1)
    out_ref[slots:rows, :] = both[0:1]

    left.wait()
    for i in range(chunk_count):
        chunks[i].wait()
        grad = jnp.dot(
            grads_v[...],
            acts_v[:, i * chunk:(i + 1) * chunk],
            preferred_element_type=jnp.float32,
        )
        addends[i].wait()
        for r in range(row_tiles):
            for c in range(chunk_blocks):
                at = i * chunk_blocks + c
                kept_ref[r, at] = residual_v[r, at] + grad[
                    r * sublanes:(r + 1) * sublanes, c * lanes:(c + 1) * lanes
                ]

    scalars.wait()
    sub = lax.broadcasted_iota(jnp.int32, (sublanes, lanes), 0)

    def pick(s, carry):
        block = index_s[0, s]
        row = block // row_blocks
        high, low, col = row // sublanes, row % sublanes, block - row * row_blocks
        out_ref[pl.ds(s, 1), :] = kept_ref[high, col, pl.ds(low, 1), :]
        mine = jnp.logical_and(sub == low, s < count)
        kept_ref[high, col] = jnp.where(mine, 0.0, kept_ref[high, col])
        return carry

    lax.fori_loop(0, slots, pick, 0, unroll=8)
    message = out_ref[0:rows, :]
    for j in range(1, members):
        out_ref[j * rows:(j + 1) * rows, :] = message


def add_kernel(held, own_ref, other_ref, *, slots, rows):
    step = slots + 1
    sources = held.shape[0] // step
    base = lax.axis_index("grp") * rows
    target = (lax.broadcasted_iota(jnp.int32, (rows, lanes), 0) + base).astype(jnp.float32)
    low = lax.broadcasted_iota(jnp.int32, (1, lanes), 1) < slots
    total = jnp.zeros((rows, 2 * lanes), jnp.float32)
    for q in range(0, sources, 4):
        hits = []
        for p in (q, q + 2):
            code = jnp.where(
                low,
                held[p * step + slots:(p + 1) * step, :],
                held[(p + 1) * step + slots:(p + 2) * step, :],
            )
            hits.append(jnp.where(target == code, 1.0, 0.0).astype(jnp.bfloat16))
        values = jnp.concatenate([held[p * step:p * step + slots, :] for p in range(q, q + 4)], axis=0)
        high = values.astype(jnp.bfloat16)
        rest = (values - high.astype(jnp.float32)).astype(jnp.bfloat16)
        total = total + jnp.dot(
            jnp.concatenate(hits, axis=1),
            jnp.concatenate([high, rest], axis=1),
            preferred_element_type=jnp.float32,
        )
    total = total[:, :lanes] + total[:, lanes:]
    part = rows // (2 * own_ref.shape[0])
    second = lax.axis_index("core") == 1
    for z in range(own_ref.shape[0]):
        even = total[2 * z * part:(2 * z + 1) * part]
        odd = total[(2 * z + 1) * part:(2 * z + 2) * part]
        own_ref[z] = jnp.where(second, odd, even)
        other_ref[z] = jnp.where(second, even, odd)


def store_kernel(kept, out_ref, sems):
    copies = [
        pltpu.make_async_copy(kept.at[i], out_ref.at[i], sems.at[i])
        for i in range(kept.shape[0])
    ]
    for copy in copies:
        copy.start()
    for copy in copies:
        copy.wait()


def join_kernel(own, other, stored, out_ref):
    out_ref[...] = own[...] + other[...]


def final_kernel(parts, momentum, out_ref):
    members, part, _ = out_ref.shape
    wide = part // sublanes * lanes
    me = lax.axis_index("grp")
    total = parts[0]
    for j in range(1, parts.shape[0]):
        total = total + parts[j]
    rows = pl.ds(pl.multiple_of((me // 2) * sublanes, sublanes), sublanes)
    old = momentum[rows, pl.ds(pl.multiple_of((me % 2) * wide, lanes), wide)]
    for c in range(part // sublanes):
        at = slice(c * sublanes, (c + 1) * sublanes)
        new = momentum_decay * old[:, c * lanes:(c + 1) * lanes] + total[at]
        for j in range(members):
            out_ref[j, at, :] = new


def in_hbm(array):
    return pltpu.with_memory_space_constraint(array, pltpu.HBM)


def local(acts, grads_out, residual_in, sel_index, sel_count, momentum_in):
    tokens, width = acts.shape
    columns = grads_out.shape[1]
    slots = sel_index.shape[1]
    row_blocks = width // lanes
    own_blocks = momentum_in.shape[1] // lanes
    members = lax.axis_size("grp")
    owners = lax.axis_size("z") * lax.axis_size("core")
    part = own_blocks // 2 * sublanes
    smem = pl.BlockSpec(memory_space=pltpu.SMEM)
    vmem = pl.BlockSpec(memory_space=pltpu.VMEM)
    hbm = pl.BlockSpec(memory_space=pl.ANY)
    tiled = residual_in.reshape(columns // sublanes, sublanes, row_blocks, lanes)
    tiled = tiled.transpose(0, 2, 1, 3)

    def pick(*refs):
        pick_kernel(*refs, row_blocks=row_blocks, own_blocks=own_blocks)

    kept, message = pl.pallas_call(
        pick,
        in_specs=[hbm, smem, hbm, hbm, hbm],
        out_specs=[vmem, vmem],
        out_shape=[
            pltpu.VMEM(tiled.shape, jnp.float32),
            pltpu.VMEM((members * (slots + 1), lanes), jnp.float32),
        ],
        scratch_shapes=[
            pltpu.SMEM((1, slots), jnp.int32),
            pltpu.VMEM((1, slots), jnp.int32),
            pltpu.VMEM((columns, tokens), jnp.bfloat16),
            pltpu.VMEM((tokens, width), jnp.bfloat16),
            pltpu.VMEM(tiled.shape, jnp.float32),
            pltpu.VMEM((sublanes, lanes), jnp.float32),
            pltpu.SemaphoreType.DMA((3,)),
            pltpu.SemaphoreType.DMA((chunk_count,)),
            pltpu.SemaphoreType.DMA((chunk_count,)),
        ],
        compiler_params=pltpu.CompilerParams(vmem_limit_bytes=16 << 20),
        name="pick",
    )(
        in_hbm(sel_index), sel_count, in_hbm(grads_out.T), in_hbm(acts), in_hbm(tiled),
    )

    held = lax.all_to_all(
        message.reshape(members, slots + 1, 1, lanes), "grp", 0, 0, tiled=True
    ).reshape(message.shape)

    shape = (lax.axis_size("z"), part, lanes)
    own, other = pl.pallas_call(
        lambda *refs: add_kernel(*refs, slots=slots, rows=owners * part),
        in_specs=[vmem],
        out_specs=[vmem, vmem],
        out_shape=[pltpu.VMEM(shape, jnp.float32), pltpu.VMEM(shape, jnp.float32)],
        compiler_params=pltpu.CompilerParams(vmem_limit_bytes=8 << 20),
        name="add",
    )(held)
    other = lax.ppermute(other, "core", [(0, 1), (1, 0)])
    kept = pl.pallas_call(
        store_kernel,
        in_specs=[vmem],
        out_specs=hbm,
        out_shape=pltpu.HBM(tiled.shape, jnp.float32),
        scratch_shapes=[pltpu.SemaphoreType.DMA((tiled.shape[0],))],
        compiler_params=pltpu.CompilerParams(vmem_limit_bytes=8 << 20),
        name="store",
    )(kept)
    sums = pl.pallas_call(
        join_kernel,
        in_specs=[vmem, vmem, hbm],
        out_specs=vmem,
        out_shape=pltpu.VMEM(shape, jnp.float32),
        compiler_params=pltpu.CompilerParams(vmem_limit_bytes=8 << 20),
        name="join",
    )(own, other, in_hbm(kept))
    parts = lax.all_to_all(sums, "z", 0, 0, tiled=True)

    new = pl.pallas_call(
        final_kernel,
        in_specs=[vmem, vmem],
        out_specs=vmem,
        out_shape=pltpu.VMEM((members, part, lanes), jnp.float32),
        compiler_params=pltpu.CompilerParams(vmem_limit_bytes=8 << 20),
        name="final",
    )(parts, momentum_in)
    whole = lax.all_to_all(new, "grp", 0, 0, tiled=True)
    whole = whole.reshape(columns // sublanes, 2, own_blocks // 2, sublanes, lanes)
    whole = whole.transpose(0, 3, 1, 2, 4).reshape(columns, own_blocks * lanes)
    kept = kept.transpose(0, 2, 1, 3).reshape(residual_in.shape)
    return (kept, whole)


def solution(mesh):
    groups, devices = mesh.devices.shape
    split = Mesh(mesh.devices.reshape(groups, devices // 2, 2), ("grp", "z", "core"))
    every = ("grp", "z", "core")
    owner = ("z", "core")
    placed = (
        P(every, None),
        P(every, None),
        P(every, None, None),
        P(every, None),
        P(every),
        P(None, owner),
    )
    return jax.shard_map(
        local,
        mesh=split,
        in_specs=placed,
        out_specs=(P(every, None, None), P(None, owner)),
        check_vma=False,
    )
```

```python
import jax
import jax.numpy as jnp
from jax import lax
from jax.experimental import pallas as pl
from jax.experimental.pallas import tpu as pltpu
from jax.sharding import Mesh
from jax.sharding import PartitionSpec as P

momentum_decay = 0.9
lanes = 128
sublanes = 8
chunk_count = 3


def pick_kernel(index, count_s, grads_t, acts, residual, grad_ref, out_ref,
                index_s, index_v, grads_v, acts_v, tiles, codes_v,
                small_sems, acts_sems, tile_sem, *, row_blocks, own_blocks):
    row_tiles = grad_ref.shape[0]
    slots = index.shape[1]
    rows = slots + 1
    members = out_ref.shape[0] // rows
    half = own_blocks // 2
    part = half * sublanes
    chunk_blocks = row_blocks // chunk_count
    chunk = chunk_blocks * lanes

    scalars = pltpu.make_async_copy(index, index_s, small_sems.at[0])
    vector = pltpu.make_async_copy(index, index_v, small_sems.at[1])
    left = pltpu.make_async_copy(grads_t, grads_v, small_sems.at[2])
    chunks = [
        pltpu.make_async_copy(
            acts.at[:, i * chunk:(i + 1) * chunk],
            acts_v.at[:, i * chunk:(i + 1) * chunk],
            acts_sems.at[i],
        )
        for i in range(chunk_count)
    ]
    scalars.start()
    left.start()
    chunks[0].start()
    vector.start()
    for copy in chunks[1:]:
        copy.start()

    def place(s):
        block = index_s[0, s]
        row = block // row_blocks
        return row // sublanes, row % sublanes, block - row * row_blocks

    def fetch(s, carry):
        high, _, col = place(s)
        pltpu.make_async_copy(residual.at[high, col], tiles.at[s], tile_sem).start()
        return carry

    scalars.wait()
    lax.fori_loop(0, slots, fetch, 0, unroll=8)

    count = count_s[0]
    vector.wait()
    block = index_v[...]
    row = (block * 43691) >> 22
    col = block - row * row_blocks
    owner = (col * 10923) >> 16
    inner = col - owner * own_blocks
    side = jnp.where(inner >= half, 1, 0)
    share = (row >> 3) * 2 + side
    target = owner * part + (inner - side * half) * sublanes + (row & 7)
    code = share * (part * row_blocks // own_blocks) + target
    slot = lax.broadcasted_iota(jnp.int32, code.shape, 1)
    code = jnp.where(slot < count, code, -1).astype(jnp.float32)
    codes_v[...] = jnp.zeros_like(codes_v)
    codes_v[0:1, 0:slots] = code
    both = codes_v[...]
    both = both + pltpu.roll(both, slots, 1)
    out_ref[slots:rows, :] = both[0:1]

    left.wait()
    for i in range(chunk_count):
        chunks[i].wait()
        grad = jnp.dot(
            grads_v[...],
            acts_v[:, i * chunk:(i + 1) * chunk],
            preferred_element_type=jnp.float32,
        )
        for r in range(row_tiles):
            for c in range(chunk_blocks):
                grad_ref[r, i * chunk_blocks + c] = grad[
                    r * sublanes:(r + 1) * sublanes, c * lanes:(c + 1) * lanes
                ]
    pltpu.make_async_copy(tiles, tiles, tile_sem).wait()

    sub = lax.broadcasted_iota(jnp.int32, (sublanes, lanes), 0)

    def pick(s, carry):
        high, low, col = place(s)
        mine = jnp.logical_and(sub == low, s < count)
        held = tiles[s]
        grad = grad_ref[high, col]
        grad_ref[high, col] = jnp.where(mine, -held, grad)
        tiles[s] = jnp.where(mine, held + grad, 0.0)
        out_ref[pl.ds(s, 1), :] = tiles[s, pl.ds(low, 1), :]
        return carry

    lax.fori_loop(0, slots, pick, 0, unroll=8)
    message = out_ref[0:rows, :]
    for j in range(1, members):
        out_ref[j * rows:(j + 1) * rows, :] = message


def add_kernel(held, own_ref, other_ref, *, slots, rows):
    step = slots + 1
    sources = held.shape[0] // step
    base = lax.axis_index("grp") * rows
    target = (lax.broadcasted_iota(jnp.int32, (rows, lanes), 0) + base).astype(jnp.float32)
    low = lax.broadcasted_iota(jnp.int32, (1, lanes), 1) < slots
    total = jnp.zeros((rows, 2 * lanes), jnp.float32)
    for q in range(0, sources, 4):
        hits = []
        for p in (q, q + 2):
            code = jnp.where(
                low,
                held[p * step + slots:(p + 1) * step, :],
                held[(p + 1) * step + slots:(p + 2) * step, :],
            )
            hits.append(jnp.where(target == code, 1.0, 0.0).astype(jnp.bfloat16))
        values = jnp.concatenate([held[p * step:p * step + slots, :] for p in range(q, q + 4)], axis=0)
        high = values.astype(jnp.bfloat16)
        rest = (values - high.astype(jnp.float32)).astype(jnp.bfloat16)
        total = total + jnp.dot(
            jnp.concatenate(hits, axis=1),
            jnp.concatenate([high, rest], axis=1),
            preferred_element_type=jnp.float32,
        )
    total = total[:, :lanes] + total[:, lanes:]
    part = rows // (2 * own_ref.shape[0])
    second = lax.axis_index("core") == 1
    for z in range(own_ref.shape[0]):
        even = total[2 * z * part:(2 * z + 1) * part]
        odd = total[(2 * z + 1) * part:(2 * z + 2) * part]
        own_ref[z] = jnp.where(second, odd, even)
        other_ref[z] = jnp.where(second, even, odd)


def join_kernel(own, other, out_ref):
    out_ref[...] = own[...] + other[...]


def final_kernel(parts, momentum, out_ref):
    members, part, _ = out_ref.shape
    wide = part // sublanes * lanes
    me = lax.axis_index("grp")
    total = parts[0]
    for j in range(1, parts.shape[0]):
        total = total + parts[j]
    rows = pl.ds(pl.multiple_of((me // 2) * sublanes, sublanes), sublanes)
    old = momentum[rows, pl.ds(pl.multiple_of((me % 2) * wide, lanes), wide)]
    for c in range(part // sublanes):
        at = slice(c * sublanes, (c + 1) * sublanes)
        new = momentum_decay * old[:, c * lanes:(c + 1) * lanes] + total[at]
        for j in range(members):
            out_ref[j, at, :] = new


def keep_kernel(grad, residual, out_ref, held, in_sems, out_sems):
    row_tiles, row_blocks, _, _ = grad.shape
    reads = [
        pltpu.make_async_copy(residual.at[i], held.at[i], in_sems.at[i])
        for i in range(row_tiles)
    ]
    writes = [
        pltpu.make_async_copy(held.at[i], out_ref.at[i], out_sems.at[i])
        for i in range(row_tiles)
    ]
    for copy in reads:
        copy.start()
    for i in range(row_tiles):
        reads[i].wait()

        def add(c, carry):
            held[i, c] = held[i, c] + grad[i, c]
            return carry

        lax.fori_loop(0, row_blocks, add, 0, unroll=16)
        writes[i].start()
    for copy in writes:
        copy.wait()


def in_hbm(array):
    return pltpu.with_memory_space_constraint(array, pltpu.HBM)


def local(acts, grads_out, residual_in, sel_index, sel_count, momentum_in):
    tokens, width = acts.shape
    columns = grads_out.shape[1]
    slots = sel_index.shape[1]
    row_blocks = width // lanes
    own_blocks = momentum_in.shape[1] // lanes
    members = lax.axis_size("grp")
    owners = lax.axis_size("z") * lax.axis_size("core")
    part = own_blocks // 2 * sublanes
    smem = pl.BlockSpec(memory_space=pltpu.SMEM)
    vmem = pl.BlockSpec(memory_space=pltpu.VMEM)
    hbm = pl.BlockSpec(memory_space=pl.ANY)
    tiled = residual_in.reshape(columns // sublanes, sublanes, row_blocks, lanes)
    tiled = tiled.transpose(0, 2, 1, 3)

    def pick(*refs):
        pick_kernel(*refs, row_blocks=row_blocks, own_blocks=own_blocks)

    grad, message = pl.pallas_call(
        pick,
        in_specs=[hbm, smem, hbm, hbm, hbm],
        out_specs=[vmem, vmem],
        out_shape=[
            pltpu.VMEM(tiled.shape, jnp.float32),
            pltpu.VMEM((members * (slots + 1), lanes), jnp.float32),
        ],
        scratch_shapes=[
            pltpu.SMEM((1, slots), jnp.int32),
            pltpu.VMEM((1, slots), jnp.int32),
            pltpu.VMEM((columns, tokens), jnp.bfloat16),
            pltpu.VMEM((tokens, width), jnp.bfloat16),
            pltpu.VMEM((slots, sublanes, lanes), jnp.float32),
            pltpu.VMEM((sublanes, lanes), jnp.float32),
            pltpu.SemaphoreType.DMA((3,)),
            pltpu.SemaphoreType.DMA((chunk_count,)),
            pltpu.SemaphoreType.DMA,
        ],
        compiler_params=pltpu.CompilerParams(vmem_limit_bytes=16 << 20),
        name="pick",
    )(
        in_hbm(sel_index), sel_count, in_hbm(grads_out.T), in_hbm(acts), in_hbm(tiled),
    )

    held = lax.all_to_all(
        message.reshape(members, slots + 1, 1, lanes), "grp", 0, 0, tiled=True
    ).reshape(message.shape)

    shape = (lax.axis_size("z"), part, lanes)
    own, other = pl.pallas_call(
        lambda *refs: add_kernel(*refs, slots=slots, rows=owners * part),
        in_specs=[vmem],
        out_specs=[vmem, vmem],
        out_shape=[pltpu.VMEM(shape, jnp.float32), pltpu.VMEM(shape, jnp.float32)],
        compiler_params=pltpu.CompilerParams(vmem_limit_bytes=8 << 20),
        name="add",
    )(held)
    other = lax.ppermute(other, "core", [(0, 1), (1, 0)])
    sums = pl.pallas_call(
        join_kernel,
        in_specs=[vmem, vmem],
        out_specs=vmem,
        out_shape=pltpu.VMEM(shape, jnp.float32),
        compiler_params=pltpu.CompilerParams(vmem_limit_bytes=8 << 20),
        name="join",
    )(own, other)
    parts = lax.all_to_all(sums, "z", 0, 0, tiled=True)

    new = pl.pallas_call(
        final_kernel,
        in_specs=[vmem, vmem],
        out_specs=vmem,
        out_shape=pltpu.VMEM((members, part, lanes), jnp.float32),
        compiler_params=pltpu.CompilerParams(vmem_limit_bytes=8 << 20),
        name="final",
    )(parts, momentum_in)
    whole = lax.all_to_all(new, "grp", 0, 0, tiled=True)
    whole = whole.reshape(columns // sublanes, 2, own_blocks // 2, sublanes, lanes)
    whole = whole.transpose(0, 3, 1, 2, 4).reshape(columns, own_blocks * lanes)
    kept = pl.pallas_call(
        keep_kernel,
        in_specs=[vmem, hbm],
        out_specs=hbm,
        out_shape=pltpu.HBM(tiled.shape, jnp.float32),
        scratch_shapes=[
            pltpu.VMEM(tiled.shape, jnp.float32),
            pltpu.SemaphoreType.DMA((tiled.shape[0],)),
            pltpu.SemaphoreType.DMA((tiled.shape[0],)),
        ],
        compiler_params=pltpu.CompilerParams(vmem_limit_bytes=8 << 20),
        name="keep",
    )(pltpu.with_memory_space_constraint(grad, pltpu.VMEM), in_hbm(tiled))
    kept = kept.transpose(0, 2, 1, 3).reshape(residual_in.shape)
    return (kept, whole)


def solution(mesh):
    groups, devices = mesh.devices.shape
    split = Mesh(mesh.devices.reshape(groups, devices // 2, 2), ("grp", "z", "core"))
    every = ("grp", "z", "core")
    owner = ("z", "core")
    placed = (
        P(every, None),
        P(every, None),
        P(every, None, None),
        P(every, None),
        P(every),
        P(None, owner),
    )
    return jax.shard_map(
        local,
        mesh=split,
        in_specs=placed,
        out_specs=(P(every, None, None), P(None, owner)),
        check_vma=False,
    )
```

```python
import jax
import jax.numpy as jnp
from jax import lax
from jax.experimental import pallas as pl
from jax.experimental.pallas import tpu as pltpu
from jax.sharding import Mesh
from jax.sharding import PartitionSpec as P

momentum_decay = 0.9
lanes = 128
sublanes = 8
chunk_count = 3


def pick_kernel(index, count_s, grads_t, acts, residual, grad_ref, out_ref,
                index_s, index_v, grads_v, acts_v, tiles, codes_v,
                small_sems, acts_sems, tile_sem, *, row_blocks, own_blocks):
    row_tiles = grad_ref.shape[0]
    slots = index.shape[1]
    rows = slots + 1
    members = out_ref.shape[0] // rows
    half = own_blocks // 2
    part = half * sublanes
    chunk_blocks = row_blocks // chunk_count
    chunk = chunk_blocks * lanes

    scalars = pltpu.make_async_copy(index, index_s, small_sems.at[0])
    vector = pltpu.make_async_copy(index, index_v, small_sems.at[1])
    left = pltpu.make_async_copy(grads_t, grads_v, small_sems.at[2])
    chunks = [
        pltpu.make_async_copy(
            acts.at[:, i * chunk:(i + 1) * chunk],
            acts_v.at[:, i * chunk:(i + 1) * chunk],
            acts_sems.at[i],
        )
        for i in range(chunk_count)
    ]
    scalars.start()
    left.start()
    chunks[0].start()
    vector.start()
    for copy in chunks[1:]:
        copy.start()

    def place(s):
        block = index_s[0, s]
        row = block // row_blocks
        return row // sublanes, row % sublanes, block - row * row_blocks

    def fetch(s, carry):
        high, _, col = place(s)
        pltpu.make_async_copy(residual.at[high, col], tiles.at[s], tile_sem).start()
        return carry

    scalars.wait()
    lax.fori_loop(0, slots, fetch, 0, unroll=8)

    count = count_s[0]
    vector.wait()
    block = index_v[...]
    row = (block * 43691) >> 22
    col = block - row * row_blocks
    owner = (col * 10923) >> 16
    inner = col - owner * own_blocks
    side = jnp.where(inner >= half, 1, 0)
    share = (row >> 3) * 2 + side
    target = owner * part + (inner - side * half) * sublanes + (row & 7)
    code = share * (part * row_blocks // own_blocks) + target
    slot = lax.broadcasted_iota(jnp.int32, code.shape, 1)
    code = jnp.where(slot < count, code, -1).astype(jnp.float32)
    codes_v[...] = jnp.zeros_like(codes_v)
    codes_v[0:1, 0:slots] = code
    both = codes_v[...]
    both = both + pltpu.roll(both, slots, 1)
    out_ref[slots:rows, :] = both[0:1]

    left.wait()
    for i in range(chunk_count):
        chunks[i].wait()
        grad = jnp.dot(
            grads_v[...],
            acts_v[:, i * chunk:(i + 1) * chunk],
            preferred_element_type=jnp.float32,
        )
        for r in range(row_tiles):
            for c in range(chunk_blocks):
                grad_ref[r, i * chunk_blocks + c] = grad[
                    r * sublanes:(r + 1) * sublanes, c * lanes:(c + 1) * lanes
                ]
    pltpu.make_async_copy(tiles, tiles, tile_sem).wait()

    sub = lax.broadcasted_iota(jnp.int32, (sublanes, lanes), 0)

    def pick(s, carry):
        high, low, col = place(s)
        mine = jnp.logical_and(sub == low, s < count)
        held = tiles[s]
        grad = grad_ref[high, col]
        grad_ref[high, col] = jnp.where(mine, -held, grad)
        tiles[s] = jnp.where(mine, held + grad, 0.0)
        out_ref[pl.ds(s, 1), :] = tiles[s, pl.ds(low, 1), :]
        return carry

    lax.fori_loop(0, slots, pick, 0, unroll=8)
    message = out_ref[0:rows, :]
    for j in range(1, members):
        out_ref[j * rows:(j + 1) * rows, :] = message


def add_kernel(held, own_ref, other_ref, *, slots, rows):
    step = slots + 1
    sources = held.shape[0] // step
    base = lax.axis_index("grp") * rows
    target = (lax.broadcasted_iota(jnp.int32, (rows, lanes), 0) + base).astype(jnp.float32)
    low = lax.broadcasted_iota(jnp.int32, (1, lanes), 1) < slots
    total = jnp.zeros((rows, 2 * lanes), jnp.float32)
    for q in range(0, sources, 4):
        hits = []
        for p in (q, q + 2):
            code = jnp.where(
                low,
                held[p * step + slots:(p + 1) * step, :],
                held[(p + 1) * step + slots:(p + 2) * step, :],
            )
            hits.append(jnp.where(target == code, 1.0, 0.0).astype(jnp.bfloat16))
        values = jnp.concatenate([held[p * step:p * step + slots, :] for p in range(q, q + 4)], axis=0)
        high = values.astype(jnp.bfloat16)
        rest = (values - high.astype(jnp.float32)).astype(jnp.bfloat16)
        total = total + jnp.dot(
            jnp.concatenate(hits, axis=1),
            jnp.concatenate([high, rest], axis=1),
            preferred_element_type=jnp.float32,
        )
    total = total[:, :lanes] + total[:, lanes:]
    part = rows // (2 * own_ref.shape[0])
    second = lax.axis_index("core") == 1
    for z in range(own_ref.shape[0]):
        even = total[2 * z * part:(2 * z + 1) * part]
        odd = total[(2 * z + 1) * part:(2 * z + 2) * part]
        own_ref[z] = jnp.where(second, odd, even)
        other_ref[z] = jnp.where(second, even, odd)


def join_kernel(own, other, out_ref):
    out_ref[...] = own[...] + other[...]


def final_kernel(parts, momentum, kept, out_ref):
    members, part, _ = out_ref.shape
    wide = part // sublanes * lanes
    me = lax.axis_index("grp")
    total = parts[0]
    for j in range(1, parts.shape[0]):
        total = total + parts[j]
    rows = pl.ds(pl.multiple_of((me // 2) * sublanes, sublanes), sublanes)
    old = momentum[rows, pl.ds(pl.multiple_of((me % 2) * wide, lanes), wide)]
    for c in range(part // sublanes):
        at = slice(c * sublanes, (c + 1) * sublanes)
        new = momentum_decay * old[:, c * lanes:(c + 1) * lanes] + total[at]
        for j in range(members):
            out_ref[j, at, :] = new


def keep_kernel(grad, residual, out_ref, held, in_sems, out_sems):
    row_tiles, row_blocks, _, _ = grad.shape
    reads = [
        pltpu.make_async_copy(residual.at[i], held.at[i], in_sems.at[i])
        for i in range(row_tiles)
    ]
    writes = [
        pltpu.make_async_copy(held.at[i], out_ref.at[i], out_sems.at[i])
        for i in range(row_tiles)
    ]
    for copy in reads:
        copy.start()
    for i in range(row_tiles):
        reads[i].wait()

        def add(c, carry):
            held[i, c] = held[i, c] + grad[i, c]
            return carry

        lax.fori_loop(0, row_blocks, add, 0, unroll=16)
        writes[i].start()
    for copy in writes:
        copy.wait()


def in_hbm(array):
    return pltpu.with_memory_space_constraint(array, pltpu.HBM)


def local(acts, grads_out, residual_in, sel_index, sel_count, momentum_in):
    tokens, width = acts.shape
    columns = grads_out.shape[1]
    slots = sel_index.shape[1]
    row_blocks = width // lanes
    own_blocks = momentum_in.shape[1] // lanes
    members = lax.axis_size("grp")
    owners = lax.axis_size("z") * lax.axis_size("core")
    part = own_blocks // 2 * sublanes
    smem = pl.BlockSpec(memory_space=pltpu.SMEM)
    vmem = pl.BlockSpec(memory_space=pltpu.VMEM)
    hbm = pl.BlockSpec(memory_space=pl.ANY)
    tiled = residual_in.reshape(columns // sublanes, sublanes, row_blocks, lanes)
    tiled = tiled.transpose(0, 2, 1, 3)

    def pick(*refs):
        pick_kernel(*refs, row_blocks=row_blocks, own_blocks=own_blocks)

    grad, message = pl.pallas_call(
        pick,
        in_specs=[hbm, smem, hbm, hbm, hbm],
        out_specs=[vmem, vmem],
        out_shape=[
            pltpu.VMEM(tiled.shape, jnp.float32),
            pltpu.VMEM((members * (slots + 1), lanes), jnp.float32),
        ],
        scratch_shapes=[
            pltpu.SMEM((1, slots), jnp.int32),
            pltpu.VMEM((1, slots), jnp.int32),
            pltpu.VMEM((columns, tokens), jnp.bfloat16),
            pltpu.VMEM((tokens, width), jnp.bfloat16),
            pltpu.VMEM((slots, sublanes, lanes), jnp.float32),
            pltpu.VMEM((sublanes, lanes), jnp.float32),
            pltpu.SemaphoreType.DMA((3,)),
            pltpu.SemaphoreType.DMA((chunk_count,)),
            pltpu.SemaphoreType.DMA,
        ],
        compiler_params=pltpu.CompilerParams(vmem_limit_bytes=16 << 20),
        name="pick",
    )(
        in_hbm(sel_index), sel_count, in_hbm(grads_out.T), in_hbm(acts), in_hbm(tiled),
    )

    held = lax.all_to_all(
        message.reshape(members, slots + 1, 1, lanes), "grp", 0, 0, tiled=True
    ).reshape(message.shape)

    shape = (lax.axis_size("z"), part, lanes)
    own, other = pl.pallas_call(
        lambda *refs: add_kernel(*refs, slots=slots, rows=owners * part),
        in_specs=[vmem],
        out_specs=[vmem, vmem],
        out_shape=[pltpu.VMEM(shape, jnp.float32), pltpu.VMEM(shape, jnp.float32)],
        compiler_params=pltpu.CompilerParams(vmem_limit_bytes=8 << 20),
        name="add",
    )(held)
    other = lax.ppermute(other, "core", [(0, 1), (1, 0)])
    sums = pl.pallas_call(
        join_kernel,
        in_specs=[vmem, vmem],
        out_specs=vmem,
        out_shape=pltpu.VMEM(shape, jnp.float32),
        compiler_params=pltpu.CompilerParams(vmem_limit_bytes=8 << 20),
        name="join",
    )(own, other)
    parts = lax.all_to_all(sums, "z", 0, 0, tiled=True)

    kept = pl.pallas_call(
        keep_kernel,
        in_specs=[vmem, hbm],
        out_specs=hbm,
        out_shape=pltpu.HBM(tiled.shape, jnp.float32),
        scratch_shapes=[
            pltpu.VMEM(tiled.shape, jnp.float32),
            pltpu.SemaphoreType.DMA((tiled.shape[0],)),
            pltpu.SemaphoreType.DMA((tiled.shape[0],)),
        ],
        compiler_params=pltpu.CompilerParams(vmem_limit_bytes=8 << 20),
        name="keep",
    )(pltpu.with_memory_space_constraint(grad, pltpu.VMEM), in_hbm(tiled))
    new = pl.pallas_call(
        final_kernel,
        in_specs=[vmem, vmem, hbm],
        out_specs=vmem,
        out_shape=pltpu.VMEM((members, part, lanes), jnp.float32),
        compiler_params=pltpu.CompilerParams(vmem_limit_bytes=8 << 20),
        name="final",
    )(parts, momentum_in, in_hbm(kept))
    whole = lax.all_to_all(new, "grp", 0, 0, tiled=True)
    whole = whole.reshape(columns // sublanes, 2, own_blocks // 2, sublanes, lanes)
    whole = whole.transpose(0, 3, 1, 2, 4).reshape(columns, own_blocks * lanes)
    kept = kept.transpose(0, 2, 1, 3).reshape(residual_in.shape)
    return (kept, whole)


def solution(mesh):
    groups, devices = mesh.devices.shape
    split = Mesh(mesh.devices.reshape(groups, devices // 2, 2), ("grp", "z", "core"))
    every = ("grp", "z", "core")
    owner = ("z", "core")
    placed = (
        P(every, None),
        P(every, None),
        P(every, None, None),
        P(every, None),
        P(every),
        P(None, owner),
    )
    return jax.shard_map(
        local,
        mesh=split,
        in_specs=placed,
        out_specs=(P(every, None, None), P(None, owner)),
        check_vma=False,
    )
```

```python
import jax
import jax.numpy as jnp
from jax import lax
from jax.experimental import pallas as pl
from jax.experimental.pallas import tpu as pltpu
from jax.sharding import Mesh
from jax.sharding import PartitionSpec as P

momentum_decay = 0.9
lanes = 128
sublanes = 8
chunk_count = 2


def pick_kernel(index, count_s, grads_t, acts, residual, grad_ref, out_ref,
                index_s, index_v, grads_v, acts_v, tiles, codes_v,
                small_sems, acts_sems, tile_sem, *, row_blocks, own_blocks):
    row_tiles = grad_ref.shape[0]
    slots = index.shape[1]
    rows = slots + 1
    members = out_ref.shape[0] // rows
    half = own_blocks // 2
    part = half * sublanes
    chunk_blocks = row_blocks // chunk_count
    chunk = chunk_blocks * lanes

    scalars = pltpu.make_async_copy(index, index_s, small_sems.at[0])
    vector = pltpu.make_async_copy(index, index_v, small_sems.at[1])
    left = pltpu.make_async_copy(grads_t, grads_v, small_sems.at[2])
    chunks = [
        pltpu.make_async_copy(
            acts.at[:, i * chunk:(i + 1) * chunk],
            acts_v.at[:, i * chunk:(i + 1) * chunk],
            acts_sems.at[i],
        )
        for i in range(chunk_count)
    ]
    scalars.start()
    left.start()
    chunks[0].start()
    vector.start()
    for copy in chunks[1:]:
        copy.start()

    def place(s):
        block = index_s[0, s]
        row = block // row_blocks
        return row // sublanes, row % sublanes, block - row * row_blocks

    def fetch(s, carry):
        high, _, col = place(s)
        pltpu.make_async_copy(residual.at[high, col], tiles.at[s], tile_sem).start()
        return carry

    scalars.wait()
    lax.fori_loop(0, slots, fetch, 0, unroll=8)

    count = count_s[0]
    vector.wait()
    block = index_v[...]
    row = (block * 43691) >> 22
    col = block - row * row_blocks
    owner = (col * 10923) >> 16
    inner = col - owner * own_blocks
    side = jnp.where(inner >= half, 1, 0)
    share = (row >> 3) * 2 + side
    target = owner * part + (inner - side * half) * sublanes + (row & 7)
    code = share * (part * row_blocks // own_blocks) + target
    slot = lax.broadcasted_iota(jnp.int32, code.shape, 1)
    code = jnp.where(slot < count, code, -1).astype(jnp.float32)
    codes_v[...] = jnp.zeros_like(codes_v)
    codes_v[0:1, 0:slots] = code
    both = codes_v[...]
    both = both + pltpu.roll(both, slots, 1)
    out_ref[slots:rows, :] = both[0:1]

    left.wait()
    for i in range(chunk_count):
        chunks[i].wait()
        grad = jnp.dot(
            grads_v[...],
            acts_v[:, i * chunk:(i + 1) * chunk],
            preferred_element_type=jnp.float32,
        )
        for r in range(row_tiles):
            for c in range(chunk_blocks):
                grad_ref[r, i * chunk_blocks + c] = grad[
                    r * sublanes:(r + 1) * sublanes, c * lanes:(c + 1) * lanes
                ]
    pltpu.make_async_copy(tiles, tiles, tile_sem).wait()

    sub = lax.broadcasted_iota(jnp.int32, (sublanes, lanes), 0)

    def pick(s, carry):
        high, low, col = place(s)
        mine = jnp.logical_and(sub == low, s < count)
        held = tiles[s]
        grad = grad_ref[high, col]
        grad_ref[high, col] = jnp.where(mine, -held, grad)
        tiles[s] = jnp.where(mine, held + grad, 0.0)
        out_ref[pl.ds(s, 1), :] = tiles[s, pl.ds(low, 1), :]
        return carry

    lax.fori_loop(0, slots, pick, 0, unroll=8)
    message = out_ref[0:rows, :]
    for j in range(1, members):
        out_ref[j * rows:(j + 1) * rows, :] = message


def add_kernel(held, own_ref, other_ref, *, slots, rows):
    step = slots + 1
    sources = held.shape[0] // step
    base = lax.axis_index("grp") * rows
    target = (lax.broadcasted_iota(jnp.int32, (rows, lanes), 0) + base).astype(jnp.float32)
    low = lax.broadcasted_iota(jnp.int32, (1, lanes), 1) < slots
    total = jnp.zeros((rows, 2 * lanes), jnp.float32)
    for q in range(0, sources, 4):
        hits = []
        for p in (q, q + 2):
            code = jnp.where(
                low,
                held[p * step + slots:(p + 1) * step, :],
                held[(p + 1) * step + slots:(p + 2) * step, :],
            )
            hits.append(jnp.where(target == code, 1.0, 0.0).astype(jnp.bfloat16))
        values = jnp.concatenate([held[p * step:p * step + slots, :] for p in range(q, q + 4)], axis=0)
        high = values.astype(jnp.bfloat16)
        rest = (values - high.astype(jnp.float32)).astype(jnp.bfloat16)
        total = total + jnp.dot(
            jnp.concatenate(hits, axis=1),
            jnp.concatenate([high, rest], axis=1),
            preferred_element_type=jnp.float32,
        )
    total = total[:, :lanes] + total[:, lanes:]
    part = rows // (2 * own_ref.shape[0])
    second = lax.axis_index("core") == 1
    for z in range(own_ref.shape[0]):
        even = total[2 * z * part:(2 * z + 1) * part]
        odd = total[(2 * z + 1) * part:(2 * z + 2) * part]
        own_ref[z] = jnp.where(second, odd, even)
        other_ref[z] = jnp.where(second, even, odd)


def join_kernel(own, other, out_ref):
    out_ref[...] = own[...] + other[...]


def final_kernel(parts, momentum, kept, out_ref):
    members, part, _ = out_ref.shape
    wide = part // sublanes * lanes
    me = lax.axis_index("grp")
    total = parts[0]
    for j in range(1, parts.shape[0]):
        total = total + parts[j]
    rows = pl.ds(pl.multiple_of((me // 2) * sublanes, sublanes), sublanes)
    old = momentum[rows, pl.ds(pl.multiple_of((me % 2) * wide, lanes), wide)]
    for c in range(part // sublanes):
        at = slice(c * sublanes, (c + 1) * sublanes)
        new = momentum_decay * old[:, c * lanes:(c + 1) * lanes] + total[at]
        for j in range(members):
            out_ref[j, at, :] = new


def keep_kernel(grad, residual, out_ref, held, in_sems, out_sems):
    row_tiles, row_blocks, _, _ = grad.shape
    reads = [
        pltpu.make_async_copy(residual.at[i], held.at[i], in_sems.at[i])
        for i in range(row_tiles)
    ]
    writes = [
        pltpu.make_async_copy(held.at[i], out_ref.at[i], out_sems.at[i])
        for i in range(row_tiles)
    ]
    for copy in reads:
        copy.start()
    for i in range(row_tiles):
        reads[i].wait()

        def add(c, carry):
            held[i, c] = held[i, c] + grad[i, c]
            return carry

        lax.fori_loop(0, row_blocks, add, 0, unroll=16)
        writes[i].start()
    for copy in writes:
        copy.wait()


def in_hbm(array):
    return pltpu.with_memory_space_constraint(array, pltpu.HBM)


def local(acts, grads_out, residual_in, sel_index, sel_count, momentum_in):
    tokens, width = acts.shape
    columns = grads_out.shape[1]
    slots = sel_index.shape[1]
    row_blocks = width // lanes
    own_blocks = momentum_in.shape[1] // lanes
    members = lax.axis_size("grp")
    owners = lax.axis_size("z") * lax.axis_size("core")
    part = own_blocks // 2 * sublanes
    smem = pl.BlockSpec(memory_space=pltpu.SMEM)
    vmem = pl.BlockSpec(memory_space=pltpu.VMEM)
    hbm = pl.BlockSpec(memory_space=pl.ANY)
    tiled = residual_in.reshape(columns // sublanes, sublanes, row_blocks, lanes)
    tiled = tiled.transpose(0, 2, 1, 3)

    def pick(*refs):
        pick_kernel(*refs, row_blocks=row_blocks, own_blocks=own_blocks)

    grad, message = pl.pallas_call(
        pick,
        in_specs=[hbm, smem, hbm, hbm, hbm],
        out_specs=[vmem, vmem],
        out_shape=[
            pltpu.VMEM(tiled.shape, jnp.float32),
            pltpu.VMEM((members * (slots + 1), lanes), jnp.float32),
        ],
        scratch_shapes=[
            pltpu.SMEM((1, slots), jnp.int32),
            pltpu.VMEM((1, slots), jnp.int32),
            pltpu.VMEM((columns, tokens), jnp.bfloat16),
            pltpu.VMEM((tokens, width), jnp.bfloat16),
            pltpu.VMEM((slots, sublanes, lanes), jnp.float32),
            pltpu.VMEM((sublanes, lanes), jnp.float32),
            pltpu.SemaphoreType.DMA((3,)),
            pltpu.SemaphoreType.DMA((chunk_count,)),
            pltpu.SemaphoreType.DMA,
        ],
        compiler_params=pltpu.CompilerParams(vmem_limit_bytes=16 << 20),
        name="pick",
    )(
        in_hbm(sel_index), sel_count, in_hbm(grads_out.T), in_hbm(acts), in_hbm(tiled),
    )

    held = lax.all_to_all(
        message.reshape(members, slots + 1, 1, lanes), "grp", 0, 0, tiled=True
    ).reshape(message.shape)

    shape = (lax.axis_size("z"), part, lanes)
    own, other = pl.pallas_call(
        lambda *refs: add_kernel(*refs, slots=slots, rows=owners * part),
        in_specs=[vmem],
        out_specs=[vmem, vmem],
        out_shape=[pltpu.VMEM(shape, jnp.float32), pltpu.VMEM(shape, jnp.float32)],
        compiler_params=pltpu.CompilerParams(vmem_limit_bytes=8 << 20),
        name="add",
    )(held)
    other = lax.ppermute(other, "core", [(0, 1), (1, 0)])
    sums = pl.pallas_call(
        join_kernel,
        in_specs=[vmem, vmem],
        out_specs=vmem,
        out_shape=pltpu.VMEM(shape, jnp.float32),
        compiler_params=pltpu.CompilerParams(vmem_limit_bytes=8 << 20),
        name="join",
    )(own, other)
    parts = lax.all_to_all(sums, "z", 0, 0, tiled=True)

    kept = pl.pallas_call(
        keep_kernel,
        in_specs=[vmem, hbm],
        out_specs=hbm,
        out_shape=pltpu.HBM(tiled.shape, jnp.float32),
        scratch_shapes=[
            pltpu.VMEM(tiled.shape, jnp.float32),
            pltpu.SemaphoreType.DMA((tiled.shape[0],)),
            pltpu.SemaphoreType.DMA((tiled.shape[0],)),
        ],
        compiler_params=pltpu.CompilerParams(vmem_limit_bytes=8 << 20),
        name="keep",
    )(pltpu.with_memory_space_constraint(grad, pltpu.VMEM), in_hbm(tiled))
    new = pl.pallas_call(
        final_kernel,
        in_specs=[vmem, vmem, hbm],
        out_specs=vmem,
        out_shape=pltpu.VMEM((members, part, lanes), jnp.float32),
        compiler_params=pltpu.CompilerParams(vmem_limit_bytes=8 << 20),
        name="final",
    )(parts, momentum_in, in_hbm(kept))
    whole = lax.all_to_all(new, "grp", 0, 0, tiled=True)
    whole = whole.reshape(columns // sublanes, 2, own_blocks // 2, sublanes, lanes)
    whole = whole.transpose(0, 3, 1, 2, 4).reshape(columns, own_blocks * lanes)
    kept = kept.transpose(0, 2, 1, 3).reshape(residual_in.shape)
    return (kept, whole)


def solution(mesh):
    groups, devices = mesh.devices.shape
    split = Mesh(mesh.devices.reshape(groups, devices // 2, 2), ("grp", "z", "core"))
    every = ("grp", "z", "core")
    owner = ("z", "core")
    placed = (
        P(every, None),
        P(every, None),
        P(every, None, None),
        P(every, None),
        P(every),
        P(None, owner),
    )
    return jax.shard_map(
        local,
        mesh=split,
        in_specs=placed,
        out_specs=(P(every, None, None), P(None, owner)),
        check_vma=False,
    )
```
